32 devices in a mesh: strip: 4 (over z), tile: 8 (over y, x, core).
Axes of the slice: x: 2, y: 2, z: 4, core: 2. Of those that a mesh axis runs over, the one named last changes fastest.
Arguments:
- coords: float32 [1536, 3, 128], P(('strip', 'tile')), may hold values from -0.25 to 1536.25, as said below
- displacement: float32 [1536, 3, 128], P(('strip', 'tile')), may hold values from -0.75 to 0.75
- pairs: int32 [2048, 2], P(('strip', 'tile')), may hold values from 0 to 1535, as said below
- intact: int32 [2048, 128, 128], P(('strip', 'tile')), may hold values 0 or 1
Outputs:
- force: float32 [1536, 3, 128], P(('strip', 'tile'))
The draws below stay inside these ranges and needn't reach their ends.
Inputs may be any that keep to these rules, and one draw needn't show every extreme that they name: `coords`: each point sits within 0.25 of its lattice site: tile t covers a 4 x 4 x 8 block of unit lattice sites starting at (4 (t // 384), 4 (t % 384), 0), point i at offset (i % 4, (i // 4) % 4, i // 16). `pairs`: the rows of one device (device number d = strip index * 8 + tile index) name as first tile one of the 48 tiles that this device holds, and as second tile a different one whose strip differs from the first's by at most one and whose place within its strip differs from the first's place within its strip by at most one.
All inputs are finite; a program needn't handle non-finite values. No bound on the sum of `intact` on one device may be relied on, other than what follows from the above.
Results may differ from the reference program's by a relative error of at most 0.0003.
Values sent between devices are 32-bit elements; how exact they have to be, the bound alone decides.
A program may use at most 64 MiB of HBM per device.

```python
import math
import jax
import jax.numpy as jnp
from jax import lax

TILE = 128
TPD = 48
PAIRS_DEV = 64
TILES_STRIP = 384
TILES = 1536
PAIRS = 2048
N_STRIP = 4
N_TILE = 8


def draw_coords(key, part):
    tile_ids = jnp.arange(TILES)[:, None]
    point_ids = jnp.arange(TILE)[None, :]
    across = 4 * (tile_ids // TILES_STRIP) + point_ids % 4
    along = 4 * (tile_ids % TILES_STRIP) + point_ids // 4 % 4
    depth = point_ids // 16 + 0 * tile_ids
    lattice = jnp.stack([across, along, depth], axis=1).astype(jnp.float32)
    jitter = jax.random.uniform(key, lattice.shape, jnp.float32, -0.2, 0.2)
    return lattice + jitter


def draw_pairs(key, part):
    keys = jax.random.split(jax.random.fold_in(key, 17), 3)
    rows = jnp.arange(PAIRS)
    strip_of = rows // (PAIRS_DEV * N_TILE)
    device_in_strip = rows // PAIRS_DEV % N_TILE
    first_local = device_in_strip * TPD + jax.random.randint(keys[0], (PAIRS,), 0, TPD)
    side = jax.random.randint(keys[1], (PAIRS,), -1, 2)
    offset = jax.random.randint(keys[2], (PAIRS,), -1, 2)
    second_strip = jnp.clip(strip_of + side, 0, N_STRIP - 1)
    second_local = jnp.clip(first_local + offset, 0, TILES_STRIP - 1)
    same = (second_strip == strip_of) & (second_local == first_local)
    moved_local = jnp.where(first_local + 1 < TILES_STRIP, first_local + 1, first_local - 1)
    second_local = jnp.where(same, moved_local, second_local)
    first_tile = strip_of * TILES_STRIP + first_local
    second_tile = second_strip * TILES_STRIP + second_local
    return jnp.stack([first_tile, second_tile], axis=1).astype(jnp.int32)


def touch_ends(drawn, rng, low, high):
    longest = drawn.shape.index(max(drawn.shape))
    spots = []
    for shift in (0, 1):
        where = [jax.random.randint(jax.random.fold_in(rng, axis), (), 0, length) for axis, length in enumerate(drawn.shape)]
        where[longest] = (where[longest] + shift) % drawn.shape[longest]
        spots.append(tuple(where))
    return drawn.at[spots[0]].set(low).at[spots[1]].set(high)


def block_scale(own_key, extent, shards, smallest, top_value):
    level = 1.0
    for position, parts in shards:
        draws = jax.random.uniform(jax.random.fold_in(jax.random.fold_in(own_key, 6), position), (parts,), jnp.float32, smallest / len(shards), top_value / len(shards))
        level = level * jnp.repeat(jnp.exp(draws), extent[position] // parts).reshape((-1,) + (1,) * (len(extent) - 1 - position))
    return level


def gaussian(rng, extent, deviation, limit, pieces=(), kind=jnp.bfloat16):
    result = deviation * jax.random.normal(rng, extent, jnp.float32)
    if pieces:
        result = result * block_scale(rng, extent, pieces, -0.22, 0.18)
    return jnp.clip(result, -limit, limit).astype(kind)


def setup_inputs(seed: int = 0) -> dict:
    key_list = jax.random.split(jax.random.key(seed), 5)
    return {
        "coords": draw_coords(jax.random.fold_in(key_list[4], 71), 0),
        "displacement": gaussian(key_list[1], (TILES, 3, TILE), 0.05, 0.75, ((0, 32),), jnp.float32),
        "pairs": draw_pairs(jax.random.fold_in(key_list[4], 71), 0),
        "intact": touch_ends((jax.random.randint(key_list[3], (PAIRS, TILE, TILE), 0, 8) < 7).astype(jnp.int32), jax.random.fold_in(key_list[3], 1), 0, 1),
    }


horizon = 3.0
stiffness = 2.0
onset_stretch = 0.02
final_stretch = 0.05

def block_forces(first_block, second, bond_mask):
    bond_ref = second[0:3, None, :] - first_block[0:3, :, None]
    bond_now = bond_ref + second[3:6, None, :] - first_block[3:6, :, None]
    length_ref = jnp.sqrt(lax.optimization_barrier(jnp.sum(bond_ref * bond_ref, axis=0)))
    length_now = jnp.sqrt(lax.optimization_barrier(jnp.sum(bond_now * bond_now, axis=0)))
    stretch = (length_now - length_ref) / length_ref
    influence = jnp.maximum(0.0, 1.0 - length_ref / horizon)
    soften = jnp.clip((final_stretch - stretch) / (final_stretch - onset_stretch), 0.0, 1.0)
    pull_scale = stiffness * stretch * influence * soften * bond_mask.astype(jnp.float32) / length_now
    bond_force = pull_scale[None] * bond_now
    return (lax.optimization_barrier(jnp.sum(bond_force, axis=2)), -lax.optimization_barrier(jnp.sum(bond_force, axis=1)))

def reference(coords, displacement, pairs, intact):
    point_table = jnp.concatenate([coords, displacement], axis=1)
    group_size = math.gcd(pairs.shape[0], 8)
    grouped_pairs = pairs.reshape(-1, group_size, 2)
    grouped_bonds = intact.reshape(-1, group_size, intact.shape[1], intact.shape[2])

    def visit(forces, scan_item):
        couple, bond_mask = scan_item
        first_ids = couple[:, 0].astype(jnp.int32)
        second_ids = couple[:, 1].astype(jnp.int32)
        gain_first, gain_second = jax.vmap(block_forces)(point_table[first_ids], point_table[second_ids], bond_mask)
        forces = forces.at[first_ids].add(gain_first)
        forces = forces.at[second_ids].add(gain_second)
        return (forces, None)
    zero_forces = jnp.zeros(coords.shape, coords.dtype)
    forces, unused = lax.scan(visit, zero_forces, (grouped_pairs, grouped_bonds))
    return forces
```

```python
import math

import jax
import jax.numpy as jnp
from jax import lax
from jax.experimental import pallas as pl
from jax.experimental.pallas import tpu as pltpu
from jax.sharding import PartitionSpec as P

horizon = 3.0
stiffness = 2.0
onset_stretch = 0.02
final_stretch = 0.05


def from_behind(value, axis, steps):
    count = lax.axis_size(axis)
    first, last = (max(0, -steps), min(count, count - steps))
    return lax.ppermute(value, axis, [(source, source + steps) for source in range(first, last)])


def padded(block, sides, width):
    for axis, dim in sides:
        count = lax.axis_size(axis)
        forward = [(i, i + 1) for i in range(count - 1)]
        backward = [(target, source) for source, target in forward]
        low = lax.ppermute(
            lax.slice_in_dim(block, block.shape[dim] - width, None, axis=dim), axis, forward
        )
        high = lax.ppermute(lax.slice_in_dim(block, 0, width, axis=dim), axis, backward)
        block = jnp.concatenate([low, block, high], axis=dim)
    return block


def strip_pass(below_part, above_part):
    from_above = from_behind(below_part, "strip", -1)
    from_below = from_behind(above_part, "strip", 1)
    return from_above + from_below


def tile_pass(left_edge, right_edge):
    to_last = from_behind(left_edge, "tile", -1)
    to_first = from_behind(right_edge, "tile", 1)
    return (to_last, to_first)


def split_rows(rows):
    row = lax.broadcasted_iota(jnp.int32, rows.shape, 0)
    lead = jnp.where(row < 3, rows, jnp.where(row == 3, 1.0, 0.0))
    high = lead.astype(jnp.bfloat16).astype(jnp.float32)
    return jnp.concatenate([high, lead - high], axis=0).astype(jnp.bfloat16)


def pair_pull(first_columns, second_rows, shift, bonds):
    def part(c):
        return second_rows[c : c + 1] + shift[c] - first_columns[:, c : c + 1]

    def norm2(c):
        x, y, z = part(c), part(c + 1), part(c + 2)
        return x * x + y * y + z * z

    now2, ref2 = norm2(0), norm2(3)
    inv_now, inv_ref = lax.rsqrt(now2), lax.rsqrt(ref2)
    ratio = now2 * inv_now * inv_ref
    influence = jnp.maximum(0.0, stiffness - ref2 * inv_ref * (stiffness / horizon))
    span = final_stretch - onset_stretch
    soften = jnp.clip((1.0 + final_stretch - ratio) * (1.0 / span), 0.0, 1.0)
    pull = (ratio - 1.0) * influence * (soften * inv_now)
    return jnp.where(bonds != 0, pull, 0.0)


def dot_rows(rows, matrix):
    return lax.dot_general(rows, matrix, (((1,), (0,)), ((), ())), preferred_element_type=jnp.float32)


def dot_columns(rows, matrix):
    return lax.dot_general(rows, matrix, (((1,), (1,)), ((), ())), preferred_element_type=jnp.float32)


def forces_kernel(group, chunk, slots_ref, table_ref, bonds_ref, forces_ref):
    step = pl.program_id(0)
    points = table_ref.shape[2]

    @pl.when(step == 0)
    def _():
        forces_ref[...] = jnp.zeros_like(forces_ref)

    def visit(i, carry):
        k = step * group + i
        first, second = slots_ref[0, k], slots_ref[1, k]
        move_x = slots_ref[2, k].astype(jnp.float32)
        move_y = slots_ref[3, k].astype(jnp.float32)
        first_rows, second_rows = table_ref[first], table_ref[second]
        shift = (move_x, move_y, 0.0, move_x, move_y, 0.0)
        columns = first_rows.T
        leads, rests = [], []
        for at in range(0, points, chunk):
            pull = pair_pull(
                columns[at : at + chunk], second_rows, shift, bonds_ref[i, at : at + chunk]
            )
            lead = pull.astype(jnp.bfloat16)
            leads.append(lead)
            rests.append((pull - lead.astype(jnp.float32)).astype(jnp.bfloat16))
        lead, rest = jnp.concatenate(leads, axis=0), jnp.concatenate(rests, axis=0)
        first_split, second_split = split_rows(first_rows), split_rows(second_rows)
        to_first = dot_columns(second_split, lead) + dot_columns(second_split, rest)
        to_second = dot_rows(first_split, lead) + dot_rows(first_split, rest)
        to_first = to_first[:8] + to_first[8:]
        to_second = to_second[:8] + to_second[8:]
        row = lax.broadcasted_iota(jnp.int32, first_rows.shape, 0)
        move = jnp.where(row == 0, move_x, jnp.where(row == 1, move_y, 0.0))
        forces_ref[first] += to_first - (first_rows - move) * to_first[3:4]
        forces_ref[second] += to_second - (second_rows + move) * to_second[3:4]
        return carry

    lax.fori_loop(0, group, visit, 0, unroll=2)


def pair_forces(slots, table, intact):
    group = math.gcd(intact.shape[0], 8)
    chunk = math.gcd(intact.shape[1], 32)
    return pl.pallas_call(
        lambda *refs: forces_kernel(group, chunk, *refs),
        grid_spec=pltpu.PrefetchScalarGridSpec(
            num_scalar_prefetch=1,
            grid=(intact.shape[0] // group,),
            in_specs=[
                pl.BlockSpec(table.shape, lambda s, slots: (0, 0, 0)),
                pl.BlockSpec((group,) + intact.shape[1:], lambda s, slots: (s, 0, 0)),
            ],
            out_specs=pl.BlockSpec(table.shape, lambda s, slots: (0, 0, 0)),
        ),
        out_shape=jax.ShapeDtypeStruct(table.shape, jnp.float32),
    )(slots, table, intact)


def on_device(coords, displacement, pairs, intact):
    per_device = coords.shape[0]
    span = per_device + 2
    points = coords.shape[-1]
    strip_tiles = per_device * lax.axis_size("tile")
    strip_index = lax.axis_index("strip")
    tile_index = lax.axis_index("tile")
    own_tiles = tile_index * per_device + jnp.arange(per_device)
    origin = jnp.stack(
        [
            jnp.full((per_device,), 4 * strip_index, jnp.int32) + 0 * own_tiles,
            4 * own_tiles,
            0 * own_tiles,
        ],
        axis=1,
    ).astype(jnp.float32)[:, :, None]
    middle = jnp.array([1.5, 1.5, 3.5], jnp.float32)[None, :, None]
    local = coords - origin - middle
    now = local + displacement
    owned = jnp.concatenate(
        [now, local, jnp.zeros((per_device, 2, points), jnp.float32)], axis=1
    )
    framed = padded(owned[None], (("strip", 0), ("tile", 1)), 1)
    framed = framed.reshape(3 * span, 8, points)
    strip_of, place_of = pairs // strip_tiles, pairs % strip_tiles
    slot = (strip_of - strip_index + 1) * span + place_of - tile_index * per_device + 1
    slots = jnp.stack(
        [
            slot[:, 0],
            slot[:, 1],
            4 * (strip_of[:, 1] - strip_of[:, 0]),
            4 * (place_of[:, 1] - place_of[:, 0]),
        ]
    )
    forces = pair_forces(slots, framed, intact)[:, :3]
    buffer = forces.reshape(3, span, 3, points)
    strip_row = buffer[1] + strip_pass(buffer[0], buffer[2])
    to_last, to_first = tile_pass(strip_row[0], strip_row[span - 1])
    result = strip_row[1 : span - 1]
    result = result.at[per_device - 1].add(to_last)
    result = result.at[0].add(to_first)
    return result


def solution(mesh):
    placed = (
        P(("strip", "tile"), None, None),
        P(("strip", "tile"), None, None),
        P(("strip", "tile"), None),
        P(("strip", "tile"), None, None),
    )
    return jax.shard_map(
        on_device,
        mesh=mesh,
        in_specs=placed,
        out_specs=P(("strip", "tile"), None, None),
        check_vma=False,
    )
```

```python
import math

import jax
import jax.numpy as jnp
from jax import lax
from jax.experimental import pallas as pl
from jax.experimental.pallas import tpu as pltpu
from jax.sharding import PartitionSpec as P

horizon = 3.0
stiffness = 2.0
onset_stretch = 0.02
final_stretch = 0.05

MESH = pl.DeviceIdType.MESH
STRIPS = (0, -1, 1)
DIRECTIONS = tuple((es, et) for es in (-1, 1, 0) for et in (0, -1, 1) if (es, et) != (0, 0))
EDGE = 8


def whole_rows(per, es):
    return pl.ds(STRIPS.index(es) * per, per)


def edge_rows(per, es, et):
    return pl.ds(3 * per + (2 * STRIPS.index(es) + (et > 0)) * EDGE, EDGE)


def split_rows(rows):
    row = lax.broadcasted_iota(jnp.int32, rows.shape, 0)
    lead = jnp.where(row < 3, rows, jnp.where(row == 3, 1.0, 0.0))
    high = lead.astype(jnp.bfloat16).astype(jnp.float32)
    return jnp.concatenate([high, lead - high], axis=0).astype(jnp.bfloat16)


def pair_pull(first, second, bonds):
    def norm2(c):
        x, y, z = (second[c + i] - first(c + i) for i in range(3))
        return x * x + y * y + z * z

    now2, ref2 = norm2(0), norm2(3)
    inv_now, inv_ref = lax.rsqrt(now2), lax.rsqrt(ref2)
    ratio = now2 * inv_now * inv_ref
    influence = jnp.maximum(0.0, stiffness - ref2 * inv_ref * (stiffness / horizon))
    span = final_stretch - onset_stretch
    soften = jnp.clip((1.0 + final_stretch) / span - ratio * (1.0 / span), 0.0, 1.0)
    pull = (ratio - 1.0) * influence * (soften * inv_now)
    return jnp.where(bonds != 0, pull, 0.0)


def dot_rows(rows, matrix):
    return lax.dot_general(rows, matrix, (((1,), (0,)), ((), ())), preferred_element_type=jnp.float32)


def dot_columns(rows, matrix):
    return lax.dot_general(rows, matrix, (((1,), (1,)), ((), ())), preferred_element_type=jnp.float32)


def force_kernel(
    scalars_ref, ends_ref, coords_ref, displacement_ref, bonds_hbm, out_ref,
    table, owned, spread, bonds, gains, forces, from_strip, from_edge,
    load_sem, send_sem, recv_sem, back_sem, home_sem,
):
    per, points = coords_ref.shape[0], coords_ref.shape[2]
    pair_count = bonds.shape[0]
    groups = load_sem.shape[0]
    group = pair_count // groups
    strip, tile = lax.axis_index("strip"), lax.axis_index("tile")
    strips, tiles = lax.axis_size("strip"), lax.axis_size("tile")

    def load(g):
        part = pl.ds(g * group, group)
        return pltpu.make_async_copy(bonds_hbm.at[part], bonds.at[part], load_sem.at[g])

    for g in range(groups):
        load(g).start()

    def exists(es, et):
        s, t = strip + es, tile + et
        return (s >= 0) & (s < strips) & (t >= 0) & (t < tiles)

    barrier = pltpu.get_barrier_semaphore()
    for es, et in DIRECTIONS:
        @pl.when(exists(es, et))
        def _(es=es, et=et):
            pl.semaphore_signal(
                barrier, inc=1, device_id=(strip + es, tile + et), device_id_type=MESH
            )

    place = lax.broadcasted_iota(jnp.int32, (per, points), 0) + tile * per
    for c in range(3):
        local = coords_ref[:, c, :]
        base = (4 * strip).astype(jnp.float32) if c == 0 else (
            4.0 * place.astype(jnp.float32) if c == 1 else 0.0)
        local = local - base - (3.5 if c == 2 else 1.5)
        table[3 + c, 0:per, :] = local
        table[c, 0:per, :] = local + displacement_ref[:, c, :]

    near = sum(
        jnp.where(exists(es, et), 1, 0) for es, et in DIRECTIONS
    )
    pl.semaphore_wait(barrier, near)

    def halo(i):
        es, et = DIRECTIONS[i]
        if et == 0:
            source, target = pl.ds(0, per), whole_rows(per, -es)
        else:
            source = pl.ds(per - EDGE if et > 0 else 0, EDGE)
            target = edge_rows(per, -es, -et)
        return pltpu.make_async_remote_copy(
            src_ref=table.at[:, source],
            dst_ref=table.at[:, target],
            send_sem=send_sem.at[i],
            recv_sem=recv_sem.at[i],
            device_id=(strip + es, tile + et),
            device_id_type=MESH,
        )

    def back(i):
        es, et = DIRECTIONS[i]
        if et == 0:
            source, target = whole_rows(per, es), from_strip.at[0 if es < 0 else 1]
        else:
            source, target = edge_rows(per, es, et), from_edge.at[i]
        return pltpu.make_async_remote_copy(
            src_ref=forces.at[:, source],
            dst_ref=target,
            send_sem=back_sem.at[i],
            recv_sem=home_sem.at[i],
            device_id=(strip + es, tile + et),
            device_id_type=MESH,
        )

    def each(step, opposite):
        for i, (es, et) in enumerate(DIRECTIONS):
            here = exists(-es, -et) if opposite else exists(es, et)
            pl.when(here)(lambda i=i: step(i))

    each(lambda i: halo(i).start(), False)

    def widen(a, carry):
        rows = [table[c, pl.ds(a, 1), :] for c in range(6)]
        row = lax.broadcasted_iota(jnp.int32, (8, points), 0)
        tall = jnp.zeros((8, points), jnp.float32)
        for c in range(6):
            tall = jnp.where(row == c, rows[c], tall)
        owned[a] = tall
        columns = tall.T
        for c in range(6):
            spread[a, c] = jnp.broadcast_to(columns[:, c : c + 1], (points, points))
        return carry

    lax.fori_loop(0, per, widen, 0, unroll=2)

    each(lambda i: halo(i).wait_recv(), True)

    chunk = math.gcd(points, 32)
    row = lax.broadcasted_iota(jnp.int32, (8, points), 0)

    def visit(k, carry):
        first, second = scalars_ref[0, k], scalars_ref[1, k]
        move_x = scalars_ref[2, k].astype(jnp.float32)
        move_y = scalars_ref[3, k].astype(jnp.float32)
        second_flat = [table[c, pl.ds(second, 1), :] for c in range(6)]
        moved = [
            second_flat[0] + move_x, second_flat[1] + move_y, second_flat[2],
            second_flat[3] + move_x, second_flat[4] + move_y, second_flat[5],
        ]
        leads, rests = [], []
        for at in range(0, points, chunk):
            pull = pair_pull(
                lambda c: spread[first, c, at : at + chunk, :], moved, bonds[k, at : at + chunk]
            )
            lead = pull.astype(jnp.bfloat16)
            leads.append(lead)
            rests.append((pull - lead.astype(jnp.float32)).astype(jnp.bfloat16))
        lead, rest = jnp.concatenate(leads, axis=0), jnp.concatenate(rests, axis=0)
        first_rows = owned[first]
        second_rows = jnp.where(
            row == 0, second_flat[0], jnp.where(row == 1, second_flat[1], second_flat[2])
        )
        first_split, second_split = split_rows(first_rows), split_rows(second_rows)
        to_first = dot_columns(second_split, lead) + dot_columns(second_split, rest)
        to_second = dot_rows(first_split, lead) + dot_rows(first_split, rest)
        to_first = to_first[:8] + to_first[8:]
        to_second = to_second[:8] + to_second[8:]
        move = jnp.where(row == 0, move_x, jnp.where(row == 1, move_y, 0.0))
        to_first = to_first - (first_rows - move) * to_first[3:4]
        to_second = to_second - (second_rows + move) * to_second[3:4]
        for c in range(3):
            gains[c, pl.ds(k, 1), :] = to_first[c : c + 1]
            gains[c, pl.ds(pair_count + k, 1), :] = to_second[c : c + 1]
        return carry

    def visit_group(g, carry):
        load(g).wait()
        return lax.fori_loop(0, group, lambda i, c: visit(g * group + i, c), carry, unroll=2)

    lax.fori_loop(0, groups, visit_group, 0)

    pieces = []
    for c in range(3):
        value = gains[c]
        for unused in range(3):
            piece = value.astype(jnp.bfloat16)
            pieces.append(piece)
            value = value - piece.astype(jnp.float32)
    pieces = jnp.concatenate(pieces, axis=1)

    def gather(start, count):
        slot = lax.broadcasted_iota(jnp.int32, (count, 2 * pair_count), 0) + start
        weight = jnp.where(slot == ends_ref[0:1, :], 1.0, 0.0).astype(jnp.bfloat16)
        sums = dot_rows(weight, pieces)
        for c in range(3):
            parts = [sums[:, (3 * c + j) * points : (3 * c + j + 1) * points] for j in range(3)]
            forces[c, start : start + count, :] = parts[0] + (parts[1] + parts[2])

    gather(per, forces.shape[1] - per)
    each(lambda i: back(i).start(), False)
    gather(0, per)

    def receive(i):
        es, et = DIRECTIONS[i]
        back(i).wait_recv()
        if et == 0:
            forces[:, 0:per, :] += from_strip[0 if es < 0 else 1]
        else:
            at = per - EDGE if et < 0 else 0
            forces[:, at : at + EDGE, :] += from_edge[i]

    each(receive, True)
    out_ref[...] = forces[:, 0:per, :]
    each(lambda i: halo(i).wait_send(), False)
    each(lambda i: back(i).wait_send(), False)


def on_device(coords, displacement, pairs, intact):
    per, points = coords.shape[0], coords.shape[2]
    pair_count = pairs.shape[0]
    groups = math.gcd(pair_count, 8)
    strip_tiles = per * lax.axis_size("tile")
    strip_index = lax.axis_index("strip")
    tile_index = lax.axis_index("tile")
    flat = pairs.T
    strip_of, place_of = flat // strip_tiles, flat % strip_tiles
    beside = strip_of - strip_index
    order = jnp.where(beside == 0, 0, jnp.where(beside < 0, 1, 2))
    at = place_of - tile_index * per
    edge = 3 * per + 2 * EDGE * order
    slot = jnp.where(at < 0, edge + EDGE - 1, jnp.where(at >= per, edge + EDGE, order * per + at))
    scalars = jnp.concatenate(
        [slot, 4 * (strip_of[1:] - strip_of[:1]), 4 * (place_of[1:] - place_of[:1])], axis=0
    )
    ends = slot.reshape(1, 2 * pair_count)
    slots = 3 * per + 6 * EDGE
    many = len(DIRECTIONS)
    vmem = pl.BlockSpec(memory_space=pltpu.VMEM)
    forces = pl.pallas_call(
        force_kernel,
        in_specs=[
            pl.BlockSpec(memory_space=pltpu.SMEM), vmem, vmem, vmem,
            pl.BlockSpec(memory_space=pl.ANY),
        ],
        out_specs=vmem,
        out_shape=jax.ShapeDtypeStruct((3, per, points), jnp.float32),
        scratch_shapes=[
            pltpu.VMEM((6, slots, points), jnp.float32),
            pltpu.VMEM((per, 8, points), jnp.float32),
            pltpu.VMEM((per, 6, points, points), jnp.float32),
            pltpu.VMEM(intact.shape, jnp.int32),
            pltpu.VMEM((3, 2 * pair_count, points), jnp.float32),
            pltpu.VMEM((3, slots, points), jnp.float32),
            pltpu.VMEM((2, 3, per, points), jnp.float32),
            pltpu.VMEM((many, 3, EDGE, points), jnp.float32),
            pltpu.SemaphoreType.DMA((groups,)),
            pltpu.SemaphoreType.DMA((many,)),
            pltpu.SemaphoreType.DMA((many,)),
            pltpu.SemaphoreType.DMA((many,)),
            pltpu.SemaphoreType.DMA((many,)),
        ],
        compiler_params=pltpu.CompilerParams(collective_id=0, has_side_effects=True),
    )(scalars, ends, coords, displacement, intact)
    return jnp.transpose(forces, (1, 0, 2))


def solution(mesh):
    placed = (
        P(("strip", "tile"), None, None),
        P(("strip", "tile"), None, None),
        P(("strip", "tile"), None),
        P(("strip", "tile"), None, None),
    )
    return jax.shard_map(
        on_device,
        mesh=mesh,
        in_specs=placed,
        out_specs=P(("strip", "tile"), None, None),
        check_vma=False,
    )
```

```python
import math

import jax
import jax.numpy as jnp
from jax import lax
from jax.experimental import pallas as pl
from jax.experimental.pallas import tpu as pltpu
from jax.sharding import PartitionSpec as P

horizon = 3.0
stiffness = 2.0
onset_stretch = 0.02
final_stretch = 0.05

MESH = pl.DeviceIdType.MESH
STRIPS = (0, -1, 1)
DIRECTIONS = tuple((es, et) for es in (-1, 1, 0) for et in (0, -1, 1) if (es, et) != (0, 0))
EDGE = 8


def whole_rows(per, es):
    return pl.ds(STRIPS.index(es) * per, per)


def edge_rows(per, es, et):
    return pl.ds(3 * per + (2 * STRIPS.index(es) + (et > 0)) * EDGE, EDGE)


def split_rows(rows):
    row = lax.broadcasted_iota(jnp.int32, rows.shape, 0)
    lead = jnp.where(row < 3, rows, jnp.where(row == 3, 1.0, 0.0))
    high = lead.astype(jnp.bfloat16).astype(jnp.float32)
    return jnp.concatenate([high, lead - high], axis=0).astype(jnp.bfloat16)


def pair_pull(first, second, bonds):
    def norm2(c):
        x, y, z = (second[c + i] - first(c + i) for i in range(3))
        return x * x + y * y + z * z

    now2, ref2 = norm2(0), norm2(3)
    inv_now, inv_ref = lax.rsqrt(now2), lax.rsqrt(ref2)
    ratio = now2 * inv_now * inv_ref
    influence = jnp.maximum(0.0, stiffness - ref2 * inv_ref * (stiffness / horizon))
    span = final_stretch - onset_stretch
    soften = jnp.clip((1.0 + final_stretch) / span - ratio * (1.0 / span), 0.0, 1.0)
    pull = (ratio - 1.0) * influence * (soften * inv_now)
    return jnp.where(bonds != 0, pull, 0.0)


def dot_rows(rows, matrix):
    return lax.dot_general(rows, matrix, (((1,), (0,)), ((), ())), preferred_element_type=jnp.float32)


def dot_columns(rows, matrix):
    return lax.dot_general(rows, matrix, (((1,), (1,)), ((), ())), preferred_element_type=jnp.float32)


def force_kernel(
    scalars_ref, ends_ref, coords_ref, displacement_ref, bonds_hbm, out_ref,
    table, owned, spread, bonds, gains, forces, from_strip, from_edge,
    load_sem, send_sem, recv_sem, back_sem, home_sem,
):
    per, points = coords_ref.shape[1], coords_ref.shape[2]
    pair_count = bonds.shape[0]
    groups = load_sem.shape[0]
    group = pair_count // groups
    strip, tile = lax.axis_index("strip"), lax.axis_index("tile")
    strips, tiles = lax.axis_size("strip"), lax.axis_size("tile")

    def load(g):
        part = pl.ds(g * group, group)
        return pltpu.make_async_copy(bonds_hbm.at[part], bonds.at[part], load_sem.at[g])

    for g in range(groups):
        load(g).start()

    def exists(es, et):
        s, t = strip + es, tile + et
        return (s >= 0) & (s < strips) & (t >= 0) & (t < tiles)

    barrier = pltpu.get_barrier_semaphore()
    for es, et in DIRECTIONS:
        @pl.when(exists(es, et))
        def _(es=es, et=et):
            pl.semaphore_signal(
                barrier, inc=1, device_id=(strip + es, tile + et), device_id_type=MESH
            )

    place = lax.broadcasted_iota(jnp.int32, (per, points), 0) + tile * per
    for c in range(3):
        local = coords_ref[c]
        base = (4 * strip).astype(jnp.float32) if c == 0 else (
            4.0 * place.astype(jnp.float32) if c == 1 else 0.0)
        local = local - base - (3.5 if c == 2 else 1.5)
        now = local + displacement_ref[c]
        table[3 + c, 0:per, :] = local
        table[c, 0:per, :] = now
        owned[:, 3 + c, :] = local
        owned[:, c, :] = now
    for c in (6, 7):
        owned[:, c, :] = jnp.zeros((per, points), jnp.float32)

    near = sum(
        jnp.where(exists(es, et), 1, 0) for es, et in DIRECTIONS
    )
    pl.semaphore_wait(barrier, near)

    def halo(i):
        es, et = DIRECTIONS[i]
        if et == 0:
            source, target = pl.ds(0, per), whole_rows(per, -es)
        else:
            source = pl.ds(per - EDGE if et > 0 else 0, EDGE)
            target = edge_rows(per, -es, -et)
        return pltpu.make_async_remote_copy(
            src_ref=table.at[:, source],
            dst_ref=table.at[:, target],
            send_sem=send_sem.at[i],
            recv_sem=recv_sem.at[i],
            device_id=(strip + es, tile + et),
            device_id_type=MESH,
        )

    def back(i):
        es, et = DIRECTIONS[i]
        if et == 0:
            source, target = whole_rows(per, es), from_strip.at[0 if es < 0 else 1]
        else:
            source, target = edge_rows(per, es, et), from_edge.at[i]
        return pltpu.make_async_remote_copy(
            src_ref=forces.at[:, source],
            dst_ref=target,
            send_sem=back_sem.at[i],
            recv_sem=home_sem.at[i],
            device_id=(strip + es, tile + et),
            device_id_type=MESH,
        )

    def each(step, opposite):
        for i, (es, et) in enumerate(DIRECTIONS):
            here = exists(-es, -et) if opposite else exists(es, et)
            pl.when(here)(lambda i=i: step(i))

    each(lambda i: halo(i).start(), False)

    def widen(g, carry):
        columns = owned[pl.ds(g * (points // 8), points // 8)].reshape(points, points).T
        for j in range(points // 8):
            for c in range(6):
                column = columns[:, 8 * j + c : 8 * j + c + 1]
                spread[g * (points // 8) + j, c] = jnp.broadcast_to(column, (points, points))
        return carry

    lax.fori_loop(0, per * 8 // points, widen, 0)

    each(lambda i: halo(i).wait_recv(), True)

    chunk = math.gcd(points, 32)
    row = lax.broadcasted_iota(jnp.int32, (8, points), 0)

    def visit(k, carry):
        first, second = scalars_ref[0, k], scalars_ref[1, k]
        move_x = scalars_ref[2, k].astype(jnp.float32)
        move_y = scalars_ref[3, k].astype(jnp.float32)
        second_flat = [table[c, pl.ds(second, 1), :] for c in range(6)]
        moved = [
            second_flat[0] + move_x, second_flat[1] + move_y, second_flat[2],
            second_flat[3] + move_x, second_flat[4] + move_y, second_flat[5],
        ]
        leads, rests = [], []
        for at in range(0, points, chunk):
            pull = pair_pull(
                lambda c: spread[first, c, at : at + chunk, :], moved, bonds[k, at : at + chunk]
            )
            lead = pull.astype(jnp.bfloat16)
            leads.append(lead)
            rests.append((pull - lead.astype(jnp.float32)).astype(jnp.bfloat16))
        lead, rest = jnp.concatenate(leads, axis=0), jnp.concatenate(rests, axis=0)
        first_rows = owned[first]
        second_rows = jnp.where(
            row == 0, second_flat[0], jnp.where(row == 1, second_flat[1], second_flat[2])
        )
        first_split, second_split = split_rows(first_rows), split_rows(second_rows)
        to_first = dot_columns(second_split, lead) + dot_columns(second_split, rest)
        to_second = dot_rows(first_split, lead) + dot_rows(first_split, rest)
        to_first = to_first[:8] + to_first[8:]
        to_second = to_second[:8] + to_second[8:]
        move = jnp.where(row == 0, move_x, jnp.where(row == 1, move_y, 0.0))
        to_first = to_first - (first_rows - move) * to_first[3:4]
        to_second = to_second - (second_rows + move) * to_second[3:4]
        for c in range(3):
            gains[c, pl.ds(k, 1), :] = to_first[c : c + 1]
            gains[c, pl.ds(pair_count + k, 1), :] = to_second[c : c + 1]
        return carry

    def visit_group(g, carry):
        load(g).wait()
        return lax.fori_loop(0, group, lambda i, c: visit(g * group + i, c), carry, unroll=2)

    lax.fori_loop(0, groups, visit_group, 0)

    def pieces_of(start):
        pieces = []
        for c in range(3):
            value = gains[c, start : start + pair_count]
            for unused in range(3):
                piece = value.astype(jnp.bfloat16)
                pieces.append(piece)
                value = value - piece.astype(jnp.float32)
        return jnp.concatenate(pieces, axis=1)

    ends = ends_ref[...]
    second_pieces = pieces_of(pair_count)

    def gather(start, count, which, pieces):
        slot = lax.broadcasted_iota(jnp.int32, (count, pair_count), 0) + start
        weight = jnp.where(slot == ends[which : which + 1], 1.0, 0.0).astype(jnp.bfloat16)
        sums = dot_rows(weight, pieces)
        for c in range(3):
            parts = [sums[:, (3 * c + j) * points : (3 * c + j + 1) * points] for j in range(3)]
            yield parts[0] + (parts[1] + parts[2])

    for c, total in enumerate(gather(per, forces.shape[1] - per, 1, second_pieces)):
        forces[c, per:, :] = total
    each(lambda i: back(i).start(), False)
    both = zip(gather(0, per, 1, second_pieces), gather(0, per, 0, pieces_of(0)))
    for c, (second_total, first_total) in enumerate(both):
        forces[c, 0:per, :] = second_total + first_total

    def receive(i):
        es, et = DIRECTIONS[i]
        back(i).wait_recv()
        if et == 0:
            forces[:, 0:per, :] += from_strip[0 if es < 0 else 1]
        else:
            at = per - EDGE if et < 0 else 0
            forces[:, at : at + EDGE, :] += from_edge[i]

    each(receive, True)
    out_ref[...] = forces[:, 0:per, :]
    each(lambda i: halo(i).wait_send(), False)
    each(lambda i: back(i).wait_send(), False)


def on_device(coords, displacement, pairs, intact):
    per, points = coords.shape[0], coords.shape[2]
    pair_count = pairs.shape[0]
    groups = math.gcd(pair_count, 8)
    strip_tiles = per * lax.axis_size("tile")
    strip_index = lax.axis_index("strip")
    tile_index = lax.axis_index("tile")
    flat = pairs.T
    strip_of, place_of = flat // strip_tiles, flat % strip_tiles
    beside = strip_of - strip_index
    order = jnp.where(beside == 0, 0, jnp.where(beside < 0, 1, 2))
    at = place_of - tile_index * per
    edge = 3 * per + 2 * EDGE * order
    slot = jnp.where(at < 0, edge + EDGE - 1, jnp.where(at >= per, edge + EDGE, order * per + at))
    listed = jnp.concatenate(
        [slot, 4 * (strip_of[1:] - strip_of[:1]), 4 * (place_of[1:] - place_of[:1])], axis=0
    )
    slots = 3 * per + 6 * EDGE
    many = len(DIRECTIONS)
    vmem = pl.BlockSpec(memory_space=pltpu.VMEM)
    forces = pl.pallas_call(
        force_kernel,
        in_specs=[
            pl.BlockSpec(memory_space=pltpu.SMEM), vmem, vmem, vmem,
            pl.BlockSpec(memory_space=pl.ANY),
        ],
        out_specs=vmem,
        out_shape=jax.ShapeDtypeStruct((3, per, points), jnp.float32),
        scratch_shapes=[
            pltpu.VMEM((6, slots, points), jnp.float32),
            pltpu.VMEM((per, 8, points), jnp.float32),
            pltpu.VMEM((per, 6, points, points), jnp.float32),
            pltpu.VMEM(intact.shape, jnp.int32),
            pltpu.VMEM((3, 2 * pair_count, points), jnp.float32),
            pltpu.VMEM((3, slots, points), jnp.float32),
            pltpu.VMEM((2, 3, per, points), jnp.float32),
            pltpu.VMEM((many, 3, EDGE, points), jnp.float32),
            pltpu.SemaphoreType.DMA((groups,)),
            pltpu.SemaphoreType.DMA((many,)),
            pltpu.SemaphoreType.DMA((many,)),
            pltpu.SemaphoreType.DMA((many,)),
            pltpu.SemaphoreType.DMA((many,)),
        ],
        compiler_params=pltpu.CompilerParams(collective_id=0, has_side_effects=True),
    )(listed, listed, coords.transpose(1, 0, 2), displacement.transpose(1, 0, 2), intact)
    return jnp.transpose(forces, (1, 0, 2))


def solution(mesh):
    placed = (
        P(("strip", "tile"), None, None),
        P(("strip", "tile"), None, None),
        P(("strip", "tile"), None),
        P(("strip", "tile"), None, None),
    )
    return jax.shard_map(
        on_device,
        mesh=mesh,
        in_specs=placed,
        out_specs=P(("strip", "tile"), None, None),
        check_vma=False,
    )
```

```python
import math

import jax
import jax.numpy as jnp
from jax import lax
from jax.experimental import pallas as pl
from jax.experimental.pallas import tpu as pltpu
from jax.sharding import PartitionSpec as P

horizon = 3.0
stiffness = 2.0
onset_stretch = 0.02
final_stretch = 0.05

MESH = pl.DeviceIdType.MESH
STRIPS = (0, -1, 1)
DIRECTIONS = tuple((es, et) for es in (-1, 1, 0) for et in (0, -1, 1) if (es, et) != (0, 0))
EDGE = 8


def whole_rows(per, es):
    return pl.ds(STRIPS.index(es) * per, per)


def edge_rows(per, es, et):
    return pl.ds(3 * per + (2 * STRIPS.index(es) + (et > 0)) * EDGE, EDGE)


def split_rows(rows):
    row = lax.broadcasted_iota(jnp.int32, rows.shape, 0)
    lead = jnp.where(row < 3, rows, jnp.where(row == 3, 1.0, 0.0))
    high = lead.astype(jnp.bfloat16).astype(jnp.float32)
    return jnp.concatenate([high, lead - high], axis=0).astype(jnp.bfloat16)


def pair_pull(first, second, bonds):
    def norm2(c):
        x, y, z = (second[c + i] - first(c + i) for i in range(3))
        return x * x + y * y + z * z

    now2, ref2 = norm2(0), norm2(3)
    inv_now, inv_ref = lax.rsqrt(now2), lax.rsqrt(ref2)
    ratio = now2 * inv_now * inv_ref
    influence = jnp.maximum(0.0, stiffness - ref2 * inv_ref * (stiffness / horizon))
    span = final_stretch - onset_stretch
    soften = jnp.clip((1.0 + final_stretch) / span - ratio * (1.0 / span), 0.0, 1.0)
    pull = (ratio - 1.0) * influence * (soften * inv_now)
    return jnp.where(bonds != 0, pull, 0.0)


def dot_rows(rows, matrix):
    return lax.dot_general(rows, matrix, (((1,), (0,)), ((), ())), preferred_element_type=jnp.float32)


def dot_columns(rows, matrix):
    return lax.dot_general(rows, matrix, (((1,), (1,)), ((), ())), preferred_element_type=jnp.float32)


def force_kernel(
    scalars_ref, ends_ref, coords_ref, displacement_ref, bonds_hbm, out_ref, received_ref,
    table, owned, spread, bonds, gains, forces, from_strip, from_edge,
    load_sem, send_sem, recv_sem, back_sem, home_sem,
):
    per, points = coords_ref.shape[1], coords_ref.shape[2]
    pair_count = bonds.shape[0]
    groups = load_sem.shape[0]
    group = pair_count // groups
    strip, tile = lax.axis_index("strip"), lax.axis_index("tile")
    strips, tiles = lax.axis_size("strip"), lax.axis_size("tile")

    def load(g):
        part = pl.ds(g * group, group)
        return pltpu.make_async_copy(bonds_hbm.at[part], bonds.at[part], load_sem.at[g])

    for g in range(groups):
        load(g).start()

    def exists(es, et):
        s, t = strip + es, tile + et
        return (s >= 0) & (s < strips) & (t >= 0) & (t < tiles)

    barrier = pltpu.get_barrier_semaphore()
    for es, et in DIRECTIONS:
        @pl.when(exists(es, et))
        def _(es=es, et=et):
            pl.semaphore_signal(
                barrier, inc=1, device_id=(strip + es, tile + et), device_id_type=MESH
            )

    place = lax.broadcasted_iota(jnp.int32, (per, points), 0) + tile * per
    for c in range(3):
        local = coords_ref[c]
        base = (4 * strip).astype(jnp.float32) if c == 0 else (
            4.0 * place.astype(jnp.float32) if c == 1 else 0.0)
        local = local - base - (3.5 if c == 2 else 1.5)
        now = local + displacement_ref[c]
        table[3 + c, 0:per, :] = local
        table[c, 0:per, :] = now
        owned[:, 3 + c, :] = local
        owned[:, c, :] = now
    for c in (6, 7):
        owned[:, c, :] = jnp.zeros((per, points), jnp.float32)

    near = sum(
        jnp.where(exists(es, et), 1, 0) for es, et in DIRECTIONS
    )
    pl.semaphore_wait(barrier, near)

    def halo(i):
        es, et = DIRECTIONS[i]
        if et == 0:
            source, target = pl.ds(0, per), whole_rows(per, -es)
        else:
            source = pl.ds(per - EDGE if et > 0 else 0, EDGE)
            target = edge_rows(per, -es, -et)
        return pltpu.make_async_remote_copy(
            src_ref=table.at[:, source],
            dst_ref=table.at[:, target],
            send_sem=send_sem.at[i],
            recv_sem=recv_sem.at[i],
            device_id=(strip + es, tile + et),
            device_id_type=MESH,
        )

    def back(i):
        es, et = DIRECTIONS[i]
        if et == 0:
            source, target = whole_rows(per, es), from_strip.at[0 if es < 0 else 1]
        else:
            source, target = edge_rows(per, es, et), from_edge.at[i]
        return pltpu.make_async_remote_copy(
            src_ref=forces.at[:, source],
            dst_ref=target,
            send_sem=back_sem.at[i],
            recv_sem=home_sem.at[i],
            device_id=(strip + es, tile + et),
            device_id_type=MESH,
        )

    def each(step, opposite):
        for i, (es, et) in enumerate(DIRECTIONS):
            here = exists(-es, -et) if opposite else exists(es, et)
            pl.when(here)(lambda i=i: step(i))

    each(lambda i: halo(i).start(), False)

    def widen(g, carry):
        columns = owned[pl.ds(g * (points // 8), points // 8)].reshape(points, points).T
        for j in range(points // 8):
            for c in range(6):
                column = columns[:, 8 * j + c : 8 * j + c + 1]
                spread[g * (points // 8) + j, c] = jnp.broadcast_to(column, (points, points))
        return carry

    lax.fori_loop(0, per * 8 // points, widen, 0)

    each(lambda i: halo(i).wait_recv(), True)

    chunk = math.gcd(points, 32)
    row = lax.broadcasted_iota(jnp.int32, (8, points), 0)

    def visit(k, carry):
        first, second = scalars_ref[0, k], scalars_ref[1, k]
        move_x = scalars_ref[2, k].astype(jnp.float32)
        move_y = scalars_ref[3, k].astype(jnp.float32)
        second_flat = [table[c, pl.ds(second, 1), :] for c in range(6)]
        moved = [
            second_flat[0] + move_x, second_flat[1] + move_y, second_flat[2],
            second_flat[3] + move_x, second_flat[4] + move_y, second_flat[5],
        ]
        leads, rests = [], []
        for at in range(0, points, chunk):
            pull = pair_pull(
                lambda c: spread[first, c, at : at + chunk, :], moved, bonds[k, at : at + chunk]
            )
            lead = pull.astype(jnp.bfloat16)
            leads.append(lead)
            rests.append((pull - lead.astype(jnp.float32)).astype(jnp.bfloat16))
        lead, rest = jnp.concatenate(leads, axis=0), jnp.concatenate(rests, axis=0)
        first_rows = owned[first]
        second_rows = jnp.where(
            row == 0, second_flat[0], jnp.where(row == 1, second_flat[1], second_flat[2])
        )
        first_split, second_split = split_rows(first_rows), split_rows(second_rows)
        to_first = dot_columns(second_split, lead) + dot_columns(second_split, rest)
        to_second = dot_rows(first_split, lead) + dot_rows(first_split, rest)
        to_first = to_first[:8] + to_first[8:]
        to_second = to_second[:8] + to_second[8:]
        move = jnp.where(row == 0, move_x, jnp.where(row == 1, move_y, 0.0))
        to_first = to_first - (first_rows - move) * to_first[3:4]
        to_second = to_second - (second_rows + move) * to_second[3:4]
        for c in range(3):
            gains[c, pl.ds(k, 1), :] = to_first[c : c + 1]
            gains[c, pl.ds(pair_count + k, 1), :] = to_second[c : c + 1]
        return carry

    def visit_group(g, carry):
        load(g).wait()
        return lax.fori_loop(0, group, lambda i, c: visit(g * group + i, c), carry, unroll=group)

    lax.fori_loop(0, groups, visit_group, 0)

    def pieces_of(start):
        pieces = []
        for c in range(3):
            value = gains[c, start : start + pair_count]
            for unused in range(3):
                piece = value.astype(jnp.bfloat16)
                pieces.append(piece)
                value = value - piece.astype(jnp.float32)
        return jnp.concatenate(pieces, axis=1)

    ends = ends_ref[...]
    second_pieces = pieces_of(pair_count)

    def gather(start, count, which, pieces):
        slot = lax.broadcasted_iota(jnp.int32, (count, pair_count), 0) + start
        weight = jnp.where(slot == ends[which : which + 1], 1.0, 0.0).astype(jnp.bfloat16)
        sums = dot_rows(weight, pieces)
        for c in range(3):
            parts = [sums[:, (3 * c + j) * points : (3 * c + j + 1) * points] for j in range(3)]
            yield parts[0] + (parts[1] + parts[2])

    for c, total in enumerate(gather(per, forces.shape[1] - per, 1, second_pieces)):
        forces[c, per:, :] = total
    each(lambda i: back(i).start(), False)
    both = zip(gather(0, per, 1, second_pieces), gather(0, per, 0, pieces_of(0)))
    for c, (second_total, first_total) in enumerate(both):
        forces[c, 0:per, :] = second_total + first_total

    def receive(i):
        es, et = DIRECTIONS[i]
        back(i).wait_recv()
        if et == 0:
            received_ref[...] += from_strip[0 if es < 0 else 1]
        else:
            at = per - EDGE if et < 0 else 0
            received_ref[:, at : at + EDGE, :] += from_edge[i]

    out_ref[...] = forces[:, 0:per, :]
    received_ref[...] = jnp.zeros_like(received_ref)
    each(receive, True)
    each(lambda i: halo(i).wait_send(), False)
    each(lambda i: back(i).wait_send(), False)


def on_device(coords, displacement, pairs, intact):
    per, points = coords.shape[0], coords.shape[2]
    pair_count = pairs.shape[0]
    groups = math.gcd(pair_count, 8)
    strip_tiles = per * lax.axis_size("tile")
    strip_index = lax.axis_index("strip")
    tile_index = lax.axis_index("tile")
    first, second = pairs.T[:1], pairs.T[1:]
    row = lax.broadcasted_iota(jnp.int32, (4, pair_count), 0)
    tiles = jnp.where(row == 0, first, second)
    beside = tiles // strip_tiles - strip_index
    order = jnp.where(beside == 0, 0, jnp.where(beside < 0, 1, 2))
    at = tiles % strip_tiles - tile_index * per
    edge = 3 * per + 2 * EDGE * order
    slot = jnp.where(at < 0, edge + EDGE - 1, jnp.where(at >= per, edge + EDGE, order * per + at))
    over = second // strip_tiles - first // strip_tiles
    along = second % strip_tiles - first % strip_tiles
    listed = jnp.where(row < 2, slot, 4 * jnp.where(row == 2, over, along))
    slots = 3 * per + 6 * EDGE
    many = len(DIRECTIONS)
    vmem = pl.BlockSpec(memory_space=pltpu.VMEM)
    own, received = pl.pallas_call(
        force_kernel,
        in_specs=[
            pl.BlockSpec(memory_space=pltpu.SMEM), vmem, vmem, vmem,
            pl.BlockSpec(memory_space=pl.ANY),
        ],
        out_specs=(vmem, vmem),
        out_shape=(jax.ShapeDtypeStruct((3, per, points), jnp.float32),) * 2,
        scratch_shapes=[
            pltpu.VMEM((6, slots, points), jnp.float32),
            pltpu.VMEM((per, 8, points), jnp.float32),
            pltpu.VMEM((per, 6, points, points), jnp.float32),
            pltpu.VMEM(intact.shape, jnp.int32),
            pltpu.VMEM((3, 2 * pair_count, points), jnp.float32),
            pltpu.VMEM((3, slots, points), jnp.float32),
            pltpu.VMEM((2, 3, per, points), jnp.float32),
            pltpu.VMEM((many, 3, EDGE, points), jnp.float32),
            pltpu.SemaphoreType.DMA((groups,)),
            pltpu.SemaphoreType.DMA((many,)),
            pltpu.SemaphoreType.DMA((many,)),
            pltpu.SemaphoreType.DMA((many,)),
            pltpu.SemaphoreType.DMA((many,)),
        ],
        compiler_params=pltpu.CompilerParams(collective_id=0, has_side_effects=True),
    )(listed, listed, coords.transpose(1, 0, 2), displacement.transpose(1, 0, 2), intact)
    return jnp.transpose(own + received, (1, 0, 2))


def solution(mesh):
    placed = (
        P(("strip", "tile"), None, None),
        P(("strip", "tile"), None, None),
        P(("strip", "tile"), None),
        P(("strip", "tile"), None, None),
    )
    return jax.shard_map(
        on_device,
        mesh=mesh,
        in_specs=placed,
        out_specs=P(("strip", "tile"), None, None),
        check_vma=False,
    )
```
